32 devices in a mesh: dp: 4 (over z), tp: 8 (over x, y, core).
Axes of the slice: x: 2, y: 2, z: 4, core: 2. Of those that a mesh axis runs over, the one named last changes fastest.
Arguments:
- x: bfloat16 [4, 2048, 512], P('dp', 'tp')
- dy: bfloat16 [4, 2048, 512], P('dp', 'tp')
- wq: bfloat16 [512, 8192], P('dp', 'tp')
- wk: bfloat16 [512, 8192], P('dp', 'tp')
- wv: bfloat16 [512, 8192], P('dp', 'tp')
- wo: bfloat16 [8192, 512], P(('tp', 'dp'))
- w_gate: bfloat16 [512, 32768], P('dp', 'tp')
- w_up: bfloat16 [512, 32768], P('dp', 'tp')
- w_down: bfloat16 [32768, 512], P(('tp', 'dp'))
Outputs:
- output 1: bfloat16 [4, 2048, 512], P('dp', 'tp')
- output 2: bfloat16 [512, 8192], P('dp', 'tp')
- output 3: bfloat16 [512, 8192], P('dp', 'tp')
- output 4: bfloat16 [512, 8192], P('dp', 'tp')
- output 5: bfloat16 [8192, 512], P(('tp', 'dp'))
- output 6: bfloat16 [512, 32768], P('dp', 'tp')
- output 7: bfloat16 [512, 32768], P('dp', 'tp')
- output 8: bfloat16 [32768, 512], P(('tp', 'dp'))
All inputs are finite; a program needn't handle non-finite values.
Results may differ from the reference program's by a relative error of at most 0.024.
Values are sent between devices in bfloat16 or wider.
A program may use at most 2 GiB of HBM per device.

```python
import jax
import jax.numpy as jnp
from jax import lax

SEQUENCES = 4
TOKENS = 2048
D = 512
HEADS = 64
KV_HEADS = 64
HEAD = 128
FF = 32768
THETA = 10000
NAMES = ("wq", "wk", "wv", "wo", "w_gate", "w_up", "w_down")
SHAPES = {
    "wq": (D, HEADS * HEAD),
    "wk": (D, KV_HEADS * HEAD),
    "wv": (D, KV_HEADS * HEAD),
    "wo": (HEADS * HEAD, D),
    "w_gate": (D, FF),
    "w_up": (D, FF),
    "w_down": (FF, D),
}


def bump(key, n, height):
    away = (jnp.arange(n, dtype=jnp.int32) - jax.random.randint(key, (), 0, n, jnp.int32)) % n
    return jnp.where(away < n // 8, height, 1.0)


def together(key, own, strength):
    shared = jax.random.normal(key, own.shape[1:], jnp.float32)
    return (own + strength * shared) * lax.rsqrt(1 + strength * strength)


def setup_inputs(seed: int = 0, part: int = 0) -> dict:
    kx, kdy, ka, kb, kz, kf, kh, kl, *kw = jax.random.split(jax.random.key(seed), 8 + len(NAMES))
    shape = (SEQUENCES, TOKENS, D)
    much_x, much_dy = jax.random.uniform(kz, (2,), jnp.float32, 0.0, 1.0)
    loud = 2.0 ** jax.random.uniform(jax.random.fold_in(kz, 1), (), jnp.float32, -1.0, 2.0)
    halves = 2.0 ** jax.random.uniform(kl, (2,), jnp.float32, -1.0, 1.0)
    times = {"wq": 1.0, "wk": 1.0, "wv": 2.0, "wo": halves[0], "w_gate": 1.0, "w_up": bump(kh, FF, 4.0), "w_down": halves[1]}
    x = together(ka, jax.random.normal(kx, shape, jnp.float32), much_x) * bump(kf, D, 4.0)
    dy = together(kb, jax.random.normal(kdy, shape, jnp.float32), much_dy)
    drawn = {"x": x.astype(jnp.bfloat16), "dy": (loud * dy * (SEQUENCES * TOKENS) ** -0.5).astype(jnp.bfloat16)}
    for key, name in zip(kw, NAMES, strict=True):
        drawn[name] = (jax.random.normal(key, SHAPES[name], jnp.float32) * SHAPES[name][0] ** -0.5 * times[name]).astype(jnp.bfloat16)
    return drawn


def matmul(a, w):
    return jnp.dot(a, w, preferred_element_type=jnp.float32).astype(jnp.bfloat16)


def normed(h):
    wide = h.astype(jnp.float32)
    scale = lax.rsqrt(jnp.mean(wide**2, -1, keepdims=True) + 1e-6)
    return (wide * scale).astype(jnp.bfloat16)


def turned(t, theta):
    half = t.shape[-1] // 2
    angle = jnp.arange(t.shape[0], dtype=jnp.float32)[:, None] * theta ** (-jnp.arange(half, dtype=jnp.float32) / half)
    cos, sin = jnp.cos(angle)[:, None], jnp.sin(angle)[:, None]
    a, b = t[..., :half].astype(jnp.float32), t[..., half:].astype(jnp.float32)
    return jnp.concatenate([a * cos - b * sin, b * cos + a * sin], -1).astype(jnp.bfloat16)


def seen_by(q, k, v):
    tokens, kv = q.shape[0], k.shape[1]
    q = q.reshape(tokens, kv, -1, q.shape[-1])
    scores = jnp.einsum("tgsd,ugd->gstu", q.astype(jnp.float32), k.astype(jnp.float32)) * q.shape[-1] ** -0.5
    place = jnp.arange(tokens)
    weights = jax.nn.softmax(jnp.where(place[:, None] >= place, scores, -jnp.inf), -1).astype(jnp.bfloat16)
    return jnp.einsum("gstu,ugd->tgsd", weights.astype(jnp.float32), v.astype(jnp.float32)).astype(jnp.bfloat16).reshape(tokens, -1)


def layer(h, w):
    a = normed(h)
    q, k = (turned(matmul(a, w[name]).reshape(h.shape[0], -1, HEAD), THETA) for name in ("wq", "wk"))
    h = h + matmul(seen_by(q, k, matmul(a, w["wv"]).reshape(h.shape[0], -1, HEAD)), w["wo"])
    b = normed(h)
    gate = jnp.dot(b, w["w_gate"], preferred_element_type=jnp.float32)
    up = jnp.dot(b, w["w_up"], preferred_element_type=jnp.float32)
    return h + matmul((jax.nn.silu(gate) * up).astype(jnp.bfloat16), w["w_down"])


def reference(x, dy, wq, wk, wv, wo, w_gate, w_up, w_down):
    weights = dict(zip(NAMES, (wq, wk, wv, wo, w_gate, w_up, w_down), strict=True))

    def take(so_far, sequence):
        h, by_y = sequence
        _, back = jax.vjp(lambda w, h: layer(h, w), weights, h)
        by_weights, by_h = back(by_y)
        return jax.tree.map(lambda total, term: total + term.astype(jnp.float32), so_far, by_weights), by_h

    none_yet = {name: jnp.zeros(w.shape, jnp.float32) for name, w in weights.items()}
    by_weights, by_x = lax.scan(take, none_yet, (x, dy))
    return (by_x, *(by_weights[name].astype(jnp.bfloat16) for name in NAMES))
```

```python
import functools

import jax
import jax.numpy as jnp
from jax import lax
from jax.experimental import pallas as pl
from jax.experimental.pallas import tpu as pltpu
from jax.sharding import PartitionSpec as P

NEG = -1e30
HIDDEN = 2 * NEG
LOG2E = 1.4426950408889634
HEAD = 128
THETA = 10000
MESH = pl.DeviceIdType.MESH
BF, F32 = jnp.bfloat16, jnp.float32
DMA, VMEM = pltpu.SemaphoreType.DMA, pltpu.VMEM
TB = 256
TILE = 2 * TB
SEQ = 2048
DM = 512
HEADS = 8
QC = HEADS * HEAD
HU = 1024
CH = 256
ROWS = 128
HBM = pl.BlockSpec(memory_space=pltpu.HBM)
LIMIT = 62 * 2**20
SCALE = HEAD**-0.5
TOP = 3
FOUR = range(4)
OTHERS = (1, 2, 3)


def _nn(a, b):
    return lax.dot_general(a, b, (((1,), (0,)), ((), ())), preferred_element_type=F32)


def _nt(a, b):
    return lax.dot_general(a, b, (((1,), (1,)), ((), ())), preferred_element_type=F32)


def _inverse(wide):
    return lax.rsqrt(jnp.mean(wide**2, -1, keepdims=True) + 1e-6)


def normed(h):
    wide = h.astype(F32)
    return (wide * _inverse(wide)).astype(BF)


def norm_back(h, grad):
    wide = h.astype(F32)
    scale = _inverse(wide)
    unit = wide * scale
    return scale * (grad - unit * jnp.mean(grad * unit, -1, keepdims=True))


BLOCK = 512


def _gap():
    return lax.broadcasted_iota(jnp.int32, (BLOCK, BLOCK), 1) - lax.broadcasted_iota(jnp.int32, (BLOCK, BLOCK), 0)


def _forward(q_ref, k_ref, v_ref, o_ref, lse_ref, top_s, mix_s):
    heads = q_ref.shape[0]
    iq = pl.program_id(0)
    e = SCALE * LOG2E
    top_s[...] = jnp.full_like(top_s, NEG)
    mix_s[...] = jnp.zeros_like(mix_s)
    ones = jnp.ones((8, BLOCK), BF)

    def block(j, masked):
        here = pl.ds(pl.multiple_of(j * BLOCK, BLOCK), BLOCK)
        scores = [_nt(k_ref[i, here, :], q_ref[i]) for i in range(heads)]
        ok = _gap() >= 0 if masked else None
        weights, keeps = [], []
        for i, s in enumerate(scores):
            if masked:
                s = jnp.where(ok, s, HIDDEN)
            old = top_s[i : i + 1, :]
            top = jnp.maximum(old, s.max(axis=0, keepdims=True))
            top_s[i : i + 1, :] = top
            weights.append(jnp.exp2((s - top) * e).astype(BF))
            keeps.append(jnp.exp2((old - top) * e))
        for i, (p, keep) in enumerate(zip(weights, keeps)):
            values = jnp.concatenate([v_ref[i, here, :].T, ones], axis=0)
            mix_s[i] = mix_s[i] * keep + _nn(values, p)

    lax.fori_loop(0, iq, lambda j, _: block(j, False), None)
    block(iq, True)
    for i in range(heads):
        total = mix_s[i, HEAD : HEAD + 1, :]
        o_ref[i] = (mix_s[i, :HEAD, :] * (1 / total)).T.astype(BF)
        lse_ref[i] = top_s[i : i + 1, :] * SCALE + jnp.log(total)


def attend(q, k, v):
    of_queries = pl.BlockSpec((HEADS, BLOCK, HEAD), lambda n: (0, n, 0))
    whole = pl.BlockSpec((HEADS, SEQ, HEAD), lambda n: (0, 0, 0))
    return pl.pallas_call(
        _forward,
        grid=(SEQ // BLOCK,),
        in_specs=[of_queries, whole, whole],
        out_specs=[of_queries, pl.BlockSpec((HEADS, 1, BLOCK), lambda n: (0, 0, n))],
        out_shape=[jax.ShapeDtypeStruct((HEADS, SEQ, HEAD), BF), jax.ShapeDtypeStruct((HEADS, 1, SEQ), F32)],
        scratch_shapes=[VMEM((HEADS, BLOCK), F32), VMEM((HEADS, HEAD + 8, BLOCK), F32)],
        compiler_params=pltpu.CompilerParams(dimension_semantics=("arbitrary",), vmem_limit_bytes=LIMIT),
        cost_estimate=pl.CostEstimate(flops=4 * HEADS * SEQ * SEQ * HEAD, transcendentals=HEADS * SEQ * SEQ, bytes_accessed=8 * HEADS * SEQ * HEAD),
        name="attend",
    )(q, k, v)


def _backward(q_ref, k_ref, v_ref, do_ref, o_ref, lse_ref, dq_ref, dk_ref, dv_ref, dq_s, dk_s, dv_s):
    heads = q_ref.shape[0]
    iq = pl.program_id(1)
    e = SCALE * LOG2E

    @pl.when(iq == 0)
    def _():
        dk_s[...] = jnp.zeros_like(dk_s)
        dv_s[...] = jnp.zeros_like(dv_s)

    dq_s[...] = jnp.zeros_like(dq_s)
    lses = [lse_ref[i] * LOG2E for i in range(heads)]
    deltas = [(do_ref[i].astype(F32) * o_ref[i].astype(F32)).T.sum(0, keepdims=True) for i in range(heads)]

    def block(j, masked):
        here = pl.ds(pl.multiple_of(j * BLOCK, BLOCK), BLOCK)
        scores = [_nt(k_ref[i, here, :], q_ref[i]) for i in range(heads)]
        dps = [_nt(v_ref[i, here, :], do_ref[i]) for i in range(heads)]
        ok = _gap() >= 0 if masked else None
        for i in range(heads):
            p = jnp.exp2(scores[i] * e - lses[i])
            if masked:
                p = jnp.where(ok, p, 0.0)
            ds = (p * (dps[i] - deltas[i])).astype(BF)
            dv_s[i, here, :] += _nn(p.astype(BF), do_ref[i])
            dk_s[i, here, :] += _nn(ds, q_ref[i])
            dq_s[i] += _nn(k_ref[i, here, :].T, ds)

    lax.fori_loop(0, iq, lambda j, _: block(j, False), None)
    block(iq, True)
    for i in range(heads):
        dq_ref[i] = (dq_s[i] * SCALE).T.astype(BF)

    @pl.when(iq == pl.num_programs(1) - 1)
    def _():
        dk_ref[...] = (dk_s[...] * SCALE).astype(BF)
        dv_ref[...] = dv_s[...].astype(BF)


def attend_back(q, k, v, d_out, out, lse):
    few = 4
    of_queries = pl.BlockSpec((few, BLOCK, HEAD), lambda h, n: (h, n, 0))
    whole = pl.BlockSpec((few, SEQ, HEAD), lambda h, n: (h, 0, 0))
    return pl.pallas_call(
        _backward,
        grid=(HEADS // few, SEQ // BLOCK),
        in_specs=[of_queries, whole, whole, of_queries, of_queries, pl.BlockSpec((few, 1, BLOCK), lambda h, n: (h, 0, n))],
        out_specs=[of_queries, whole, whole],
        out_shape=[jax.ShapeDtypeStruct((HEADS, SEQ, HEAD), BF)] * 3,
        scratch_shapes=[VMEM((few, HEAD, BLOCK), F32), VMEM((few, SEQ, HEAD), F32), VMEM((few, SEQ, HEAD), F32)],
        compiler_params=pltpu.CompilerParams(dimension_semantics=("arbitrary", "arbitrary"), vmem_limit_bytes=LIMIT),
        cost_estimate=pl.CostEstimate(flops=10 * HEADS * SEQ * SEQ * HEAD, transcendentals=HEADS * SEQ * SEQ, bytes_accessed=18 * HEADS * SEQ * HEAD),
        name="attend_back",
    )(q, k, v, d_out, out, lse)


def _flip(a, by):
    return a + by - 2 * a * by


def _chip(t, j):
    x, y = lax.div(t, 4), lax.rem(lax.div(t, 2), 2)
    return 2 * _flip(x, lax.div(j, 2)) + _flip(y, lax.rem(j, 2))


def _send(src, dst, s, r, to):
    return pltpu.make_async_remote_copy(src_ref=src, dst_ref=dst, send_sem=s, recv_sem=r, device_id=to, device_id_type=MESH)


def _meet(d, t):
    core = lax.rem(t, 2)
    barrier = pltpu.get_barrier_semaphore()
    for k in range(1, 4):
        pl.semaphore_signal(barrier, inc=1, device_id=(lax.rem(d + k, 4), t), device_id_type=MESH)
        pl.semaphore_signal(barrier, inc=1, device_id=(d, 2 * _chip(t, k) + core), device_id_type=MESH)
    pl.semaphore_signal(barrier, inc=1, device_id=(d, t + 1 - 2 * core), device_id_type=MESH)
    pl.semaphore_wait(barrier, 7)


def _params(number):
    return pltpu.CompilerParams(collective_id=number, has_side_effects=True, vmem_limit_bytes=LIMIT)


class _Gather:
    @staticmethod
    def sems(*lead):
        return [DMA((*lead, n)) for n in (3, 3, 4, 4)]

    def __init__(self, d, t, slots, xs, xr, cs, cr):
        core = lax.rem(t, 2)
        peer = lambda j: 2 * _chip(t, j) + core
        self.across = lambda j: _send(slots.at[t], slots.at[t], xs.at[j - 1], xr.at[j - 1], (d, peer(j)))
        self.to_mate = lambda j: _send(slots.at[peer(j)], slots.at[peer(j)], cs.at[j], cr.at[j], (d, t + 1 - 2 * core))

    def start(self):
        for j in OTHERS[::-1]:
            self.across(j).start()
        self.to_mate(0).start()

    def relay(self, j):
        self.across(j).wait_recv()
        self.to_mate(j).start()

    def arrived(self, j):
        self.to_mate(j).wait_recv()

    def close(self):
        for j in FOUR:
            self.to_mate(j).wait_send()
            if j:
                self.across(j).wait_send()


class _Scatter:
    @staticmethod
    def scratch(n):
        tile = lambda *lead: VMEM((*lead, TB, DM), BF)
        return [VMEM((2, TB, DM), F32), VMEM((TB, DM), F32), VMEM((n, TB, DM), F32), tile(4 * n), tile(4 * n), tile(n, 3), tile(n, 3),
                DMA((4 * n,)), DMA((4 * n,)), DMA((n, 3)), DMA((n, 3))]

    def __init__(self, d, t, n, tile, mine, keep, ps, cr, qs, xr, p_s, p_r, q_s, q_r):
        self.core = core = lax.rem(t, 2)
        self.n, self.tile, self.mine, self.keep, self.ps, self.cr, self.qs, self.xr = n, tile, mine, keep, ps, cr, qs, xr
        self.half = lambda s: _send(ps.at[s], cr.at[s], p_s.at[s], p_r.at[s], (d, t + 1 - 2 * core))
        self.quarter = lambda k, j: _send(qs.at[k, j - 1], xr.at[k, j - 1], q_s.at[k, j - 1], q_r.at[k, j - 1], (d, 2 * _chip(t, j) + core))

    def give(self, s, first=0):
        @pl.when(s > first)
        def _():
            self.settle(jnp.maximum(s - 1, first))

        self.ps[s] = self.tile[1 - self.core].astype(BF)
        self.half(s).start()
        self.mine[...] = self.tile[self.core]

    def settle(self, s):
        k, j = lax.div(s, 4), TOP - lax.rem(s, 4)
        self.half(s).wait_recv()
        total = self.mine[...] + self.cr[s].astype(F32)

        @pl.when(j > 0)
        def _():
            self.qs[k, jnp.maximum(j - 1, 0)] = total.astype(BF)
            self.quarter(k, jnp.maximum(j, 1)).start()

        @pl.when(j == 0)
        def _():
            self.keep[k] = total

    def finish(self, k):
        total = self.keep[k]
        for j in OTHERS:
            self.quarter(k, j).wait_recv()
            total += self.xr[k, j - 1].astype(F32)
        return total

    def close(self):
        for k in range(self.n):
            for j in OTHERS:
                self.quarter(k, j).wait_send()
            for i in FOUR:
                self.half(4 * k + i).wait_send()


def _spun(t, cos, sin):
    return t * cos + pltpu.roll(t, HEAD // 2, 1) * sin


def _into(a_ref, dy_ref, wq_ref, wk_ref, wv_ref, wo_ref, freq_ref, q_ref, k_ref, v_ref, ag_ref, dg_ref, wf_ref, of_ref, cos_ref, sin_ref,
          ag, dg, wf, of, cos, sin, out, ld, st, os, up_s, up_r, dn_s, dn_r, *sems):
    d, t = lax.axis_index("dp"), lax.axis_index("tp")
    of_a, of_dy = sems[:4], sems[4:]
    gather = _Gather(d, t, ag, *of_a)
    spread = lambda o: _Gather(d, t, dg.at[o], *(x.at[o] for x in of_dy))

    def block(m, o):
        if m == 0:
            return dg.at[o, t]
        step = TB if m == 4 else ROWS
        rows = pl.ds(pl.multiple_of(o * step, step), step)
        return of.at[rows] if m == 4 else wf.at[m - 1, rows]

    parts = range(5)
    loads = [pltpu.make_async_copy(source, block(m, d), ld.at[m]) for m, source in enumerate((dy_ref, wq_ref, wk_ref, wv_ref, wo_ref))]
    loads += [pltpu.make_async_copy(a_ref, ag.at[t], ld.at[5])]
    for copy in loads:
        copy.start()
    up = lambda m, o: _send(block(m, o), block(m, o), up_s.at[m, o], up_r.at[m, o], (jnp.minimum(d + 1, TOP), t))
    down = lambda m, o: _send(block(m, o), block(m, o), dn_s.at[m, o], dn_r.at[m, o], (jnp.maximum(d - 1, 0), t))
    _meet(d, t)
    for m in parts:
        loads[m].wait()

        @pl.when(d < TOP)
        def _():
            up(m, d).start()

        @pl.when(d > 0)
        def _():
            down(m, d).start()

    loads[5].wait()
    gather.start()
    spread(d).start()
    angle = lax.broadcasted_iota(jnp.int32, (SEQ, HEAD), 0).astype(F32) * freq_ref[...]
    cos[...] = jnp.cos(angle)
    sin[...] = jnp.where(lax.broadcasted_iota(jnp.int32, (SEQ, HEAD), 1) < HEAD // 2, -1.0, 1.0) * jnp.sin(angle)
    leaving = [pltpu.make_async_copy(cos, cos_ref, st.at[0]), pltpu.make_async_copy(sin, sin_ref, st.at[1])]
    for copy in leaving:
        copy.start()

    def whole(source, target, n):
        leaving.append(pltpu.make_async_copy(source, target, st.at[n]))
        leaving[-1].start()

    tokens = lambda n: pl.ds(pl.multiple_of(n * TILE, TILE), TILE)
    targets = (None, q_ref, k_ref, v_ref)
    leave = lambda m, n: pltpu.make_async_copy(out.at[m - 1, :, tokens(n)], targets[m].at[:, tokens(n)], os.at[m - 1, n])

    def multiply(m):
        def tile(n, _):
            got = _nn(ag[pl.ds(2 * n, 2)].reshape(TILE, DM), wf[m - 1]).astype(BF)
            for h in range(HEADS):
                piece = got[:, h * HEAD : (h + 1) * HEAD]
                if m < 3:
                    piece = _spun(piece.astype(F32), cos[tokens(n), :], sin[tokens(n), :]).astype(BF)
                out[m - 1, h, tokens(n), :] = piece
            leave(m, n).start()

        lax.fori_loop(0, 4, tile, None)

    for j in OTHERS:
        gather.relay(j)
    for j in FOUR:
        gather.arrived(j)
    whole(ag, ag_ref, 2)
    for far in OTHERS:
        below, above = jnp.maximum(d - far, 0), jnp.minimum(d + far, TOP)
        for m in parts:

            @pl.when(d >= far)
            def _():
                up(m, below).wait_recv()

                @pl.when(d < TOP)
                def _():
                    up(m, below).start()

                if m == 0:
                    spread(below).start()

            @pl.when(d + far <= TOP)
            def _():
                down(m, above).wait_recv()

                @pl.when(d > 0)
                def _():
                    down(m, above).start()

                if m == 0:
                    spread(above).start()

            if far == 3 and 0 < m < 4:
                multiply(m)
    whole(wf, wf_ref, 3)
    whole(of, of_ref, 4)
    for j in OTHERS:
        spread(d).relay(j)
    for far in OTHERS:
        for on, o in ((d >= far, jnp.maximum(d - far, 0)), (d + far <= TOP, jnp.minimum(d + far, TOP))):

            @pl.when(on)
            def _():
                for j in OTHERS:
                    spread(o).relay(j)

    for o in FOUR:
        for j in FOUR:
            spread(o).arrived(j)
    whole(dg, dg_ref, 5)
    for m in parts:
        if 0 < m < 4:
            for n in FOUR:
                leave(m, n).wait()
        for o in FOUR:

            @pl.when((o <= d) & (d < TOP))
            def _():
                up(m, o).wait_send()

            @pl.when((o >= d) & (d > 0))
            def _():
                down(m, o).wait_send()

    for copy in leaving:
        copy.wait()
    gather.close()
    for o in FOUR:
        spread(o).close()


def into(a, dy, wq, wk, wv, wo):
    freq = (THETA ** (-(jnp.arange(HEAD, dtype=F32) % (HEAD // 2)) / (HEAD // 2)))[None]
    heads = jax.ShapeDtypeStruct((HEADS, SEQ, HEAD), BF)
    table = jax.ShapeDtypeStruct((SEQ, HEAD), F32)
    shapes = (8, TB, DM), (4, 8, TB, DM), (3, DM, QC), (QC, DM)
    return pl.pallas_call(
        _into,
        in_specs=[HBM] * 6 + [pl.BlockSpec(memory_space=VMEM)],
        out_specs=[HBM] * 9,
        out_shape=[heads, heads, heads, *[jax.ShapeDtypeStruct(shape, BF) for shape in shapes], table, table],
        scratch_shapes=[*[VMEM(shape, BF) for shape in shapes], VMEM((SEQ, HEAD), F32), VMEM((SEQ, HEAD), F32), VMEM((3, HEADS, SEQ, HEAD), BF),
                        DMA((6,)), DMA((6,)), DMA((3, 4)), *[DMA((5, 4))] * 4, *_Gather.sems(), *_Gather.sems(4)],
        compiler_params=_params(0),
        cost_estimate=pl.CostEstimate(flops=6 * SEQ * DM * QC, transcendentals=0, bytes_accessed=24 * 2**20),
        name="into",
    )(a, dy, wq, wk, wv, wo, freq)


def _outof(dq_ref, dk_ref, dv_ref, ag_ref, wf_ref, cos_ref, sin_ref, da_ref, dw_ref,
           grads, ag, wf, cos, sin, acc, us, ds, ur, dr, ld, up_s, up_r, dn_s, dn_r, *sums):
    d, t = lax.axis_index("dp"), lax.axis_index("tp")
    scatter = _Scatter(d, t, 1, *sums)
    loads = [pltpu.make_async_copy(s, to, ld.at[n]) for n, (s, to) in enumerate(
        [(dq_ref, grads.at[0]), (ag_ref, ag), (cos_ref, cos), (sin_ref, sin), (dk_ref, grads.at[1]), (dv_ref, grads.at[2]), (wf_ref, wf)])]
    for copy in loads:
        copy.start()
    up = lambda m, p: _send(us.at[m, p], ur.at[m, p], up_s.at[m, p], up_r.at[m, p], (jnp.minimum(d + 1, TOP), t))
    down = lambda m, p: _send(ds.at[m, p], dr.at[m, p], dn_s.at[m, p], dn_r.at[m, p], (jnp.maximum(d - 1, 0), t))
    rows = lambda p: slice(p * ROWS, (p + 1) * ROWS)
    _meet(d, t)
    for copy in loads[:4]:
        copy.wait()
    for m in range(3):
        if m:
            loads[3 + m].wait()
        acc[m] = jnp.zeros_like(acc[m])

        def tile(n, _):
            place = pl.ds(pl.multiple_of(n * TILE, TILE), TILE)
            pieces = []
            for h in range(HEADS):
                piece = grads[m, h, place, :]
                if m < 2:
                    piece = _spun(piece.astype(F32), cos[place, :], -sin[place, :]).astype(BF)
                    grads[m, h, place, :] = piece
                pieces.append(piece)
            acc[m] += _nn(ag[pl.ds(2 * n, 2)].reshape(TILE, DM).T, jnp.concatenate(pieces, 1))

        lax.fori_loop(0, 4, tile, None)

        @pl.when(d == 0)
        def _():
            for p in (3, 2, 1):
                us[m, p] = acc[m, rows(p), :].astype(BF)
                up(m, p).start()

        @pl.when(d == TOP)
        def _():
            for p in (0, 1, 2):
                ds[m, p] = acc[m, rows(p), :].astype(BF)
                down(m, p).start()

    def pass_on(m):
        for n in range(3):
            p, o = 3 - n, n

            @pl.when((d > 0) & (d < p))
            def _():
                up(m, p).wait_recv()
                us[m, p] = (acc[m, rows(p), :] + ur[m, p].astype(F32)).astype(BF)
                up(m, p).start()

            @pl.when((d < TOP) & (d > o))
            def _():
                down(m, o).wait_recv()
                ds[m, o] = (acc[m, rows(o), :] + dr[m, o].astype(F32)).astype(BF)
                down(m, o).start()

    loads[6].wait()
    pass_on(0)

    def for_a(s, _):
        chip = _chip(t, 3 - s)
        place = pl.ds(pl.multiple_of(chip * TILE, TILE), TILE)
        total = sum(_nt(jnp.concatenate([grads[m, h, place, :] for h in range(HEADS)], 1), wf[m]) for m in range(3))
        scatter.tile[...] = total.reshape(2, TB, DM)
        scatter.give(s)

    lax.fori_loop(0, 4, for_a, None)
    scatter.settle(3)
    pass_on(1)
    pass_on(2)
    da_ref[...] = scatter.finish(0)
    own = pl.ds(pl.multiple_of(d * ROWS, ROWS), ROWS)
    for m in range(3):

        @pl.when(d > 0)
        def _():
            up(m, d).wait_recv()
            acc[m, own, :] += ur[m, d].astype(F32)

        @pl.when(d < TOP)
        def _():
            down(m, d).wait_recv()
            acc[m, own, :] += dr[m, d].astype(F32)

        dw_ref[m] = acc[m, own, :].astype(BF)
        for p in FOUR:

            @pl.when(d < p)
            def _():
                up(m, p).wait_send()

            @pl.when(d > p)
            def _():
                down(m, p).wait_send()

    scatter.close()


def outof(dq, dk, dv, a, weights, cos, sin):
    vmem = pl.BlockSpec(memory_space=VMEM)
    return pl.pallas_call(
        _outof,
        in_specs=[HBM] * 7,
        out_specs=[vmem] * 2,
        out_shape=[jax.ShapeDtypeStruct((TB, DM), F32), jax.ShapeDtypeStruct((3, ROWS, QC), BF)],
        scratch_shapes=[VMEM((3, HEADS, SEQ, HEAD), BF), VMEM((8, TB, DM), BF), VMEM((3, DM, QC), BF), VMEM((SEQ, HEAD), F32), VMEM((SEQ, HEAD), F32),
                        VMEM((3, DM, QC), F32), *[VMEM((3, 4, ROWS, QC), BF)] * 4, DMA((7,)), *[DMA((3, 4))] * 4, *_Scatter.scratch(1)],
        compiler_params=_params(2),
        cost_estimate=pl.CostEstimate(flops=12 * SEQ * DM * QC, transcendentals=0, bytes_accessed=24 * 2**20),
        name="outof",
    )(dq, dk, dv, a, weights, cos, sin)


def _between(o_ref, wo_ref, x_ref, h_ref, b_ref, wo, ob, ld, o_m, *sums):
    d, t = lax.axis_index("dp"), lax.axis_index("tp")
    scatter = _Scatter(d, t, 1, *sums)
    load = pltpu.make_async_copy(wo_ref, wo, ld.at[0])

    def fetch(i):
        tokens = pl.ds(pl.multiple_of(_chip(t, 3 - i) * TILE, TILE), TILE)
        return pltpu.make_async_copy(o_ref.at[:, tokens], ob.at[i], o_m.at[i])

    load.start()
    for i in FOUR:
        fetch(i).start()
    _meet(d, t)
    load.wait()

    def tile(i, _):
        fetch(i).wait()
        heads = jnp.concatenate([ob[i, h] for h in range(HEADS)], 1)
        scatter.tile[...] = _nn(heads, wo[...]).reshape(2, TB, DM)
        scatter.give(i)

    lax.fori_loop(0, 4, tile, None)
    scatter.settle(3)
    h = x_ref[...] + scatter.finish(0).astype(BF)
    h_ref[...] = h
    b_ref[...] = normed(h)
    scatter.close()


def between(o, wo, x):
    vmem = pl.BlockSpec(memory_space=VMEM)
    return pl.pallas_call(
        _between,
        in_specs=[HBM, HBM, vmem],
        out_specs=[vmem, vmem],
        out_shape=[jax.ShapeDtypeStruct((TB, DM), BF)] * 2,
        scratch_shapes=[VMEM((QC, DM), BF), VMEM((4, HEADS, TILE, HEAD), BF), DMA((1,)), DMA((4,)), *_Scatter.scratch(1)],
        compiler_params=_params(3),
        cost_estimate=pl.CostEstimate(flops=2 * SEQ * DM * QC, transcendentals=0, bytes_accessed=8 * 2**20),
        name="between",
    )(o, wo, x)


def _mlp(b_ref, h_ref, wo_ref, own_dy_ref, dy_ref, *rest):
    pieces, wd_ref = rest[:4], rest[4]
    dh_ref, dhg_ref, do_ref, ogu_ref, od_ref = rest[5:10]
    (g, dhg, wo, dyb, wgu, wd, acc, acc_d, rs, zr, out, ld, dy_m, st, zs_s, zs_r, r_s, r_r) = rest[10:28]
    sems, sums = rest[28:36], rest[36:]
    d, t = lax.axis_index("dp"), lax.axis_index("tp")
    place = lambda k: lax.rem(d + k, 4)
    scatter = _Scatter(d, t, 4, *sums)
    along_z = lambda k: _send(g.at[0, t], g.at[k, t], zs_s.at[k - 1], zs_r.at[k - 1], (lax.rem(d - k + 4, 4), t))
    gather = lambda k: _Gather(d, t, g.at[k], *(x.at[k] for x in sems[:4]))
    home = lambda k: _send(rs.at[k - 1], zr.at[k - 1], r_s.at[k - 1], r_r.at[k - 1], (place(k), t))
    tokens = lambda chip: pl.ds(pl.multiple_of(chip * TILE, TILE), TILE)

    def fetch(s):
        k, j = lax.div(s, 4), TOP - lax.rem(s, 4)
        return pltpu.make_async_copy(dy_ref.at[place(k), _chip(t, j)], dyb.at[lax.rem(s, 2)], dy_m.at[lax.rem(s, 2)])

    loads = [pltpu.make_async_copy(b_ref, g.at[0, t], ld.at[0]), pltpu.make_async_copy(wd_ref, wd, ld.at[1])]
    for k in FOUR:
        rows = pl.ds(pl.multiple_of(place(k) * ROWS, ROWS), ROWS)
        loads += [pltpu.make_async_copy(pieces[k], wgu.at[:, rows], ld.at[2 + k])]
    loads += [pltpu.make_async_copy(wo_ref, wo, ld.at[6])]
    for copy in loads:
        copy.start()
    fetch(0).start()
    _meet(d, t)
    loads[0].wait()
    gather(0).start()
    for k in OTHERS:
        along_z(k).start()
    acc[...] = jnp.zeros_like(acc)
    acc_d[...] = jnp.zeros_like(acc_d)
    along_z(1).wait_recv()
    gather(1).start()
    for copy in loads[1:]:
        copy.wait()
    for j in OTHERS:
        gather(0).relay(j)

    def step(s, _):
        k, i = lax.div(s, 4), lax.rem(s, 4)
        chip = _chip(t, 3 - i)
        after = jnp.minimum(k + 1, 3)

        @pl.when(i == 0)
        def _():
            for n in FOUR:
                gather(k).arrived(n)

        @pl.when((s == 1) | (s == 2))
        def _():
            n = jnp.clip(s + 1, 2, 3)
            along_z(n).wait_recv()
            gather(n).start()

        @pl.when((i == 3) & (k < TOP))
        def _():
            for n in OTHERS:
                gather(after).relay(n)

        @pl.when(s < 15)
        def _():
            fetch(s + 1).start()

        fetch(s).wait()
        bt = g[k, pl.ds(2 * chip, 2)].reshape(TILE, DM)
        dyt = dyb[lax.rem(s, 2)]
        bx, dyx = bt.T, dyt.T
        db = None
        for n in range(HU // CH):
            at = slice(n * CH, (n + 1) * CH)
            gate, up = _nn(bt, wgu[0, :, at]), _nn(bt, wgu[1, :, at])
            dh = _nt(dyt, wd[at, :]).astype(BF).astype(F32)
            sig = 1 / (1 + jnp.exp(-gate))
            act = gate * sig
            hid = (act * up).astype(BF)
            du = (dh * act).astype(BF)
            dg = (dh * up * (sig * (1 + gate * (1 - sig)))).astype(BF)
            acc[0, :, at] += _nn(bx, dg)
            acc[1, :, at] += _nn(bx, du)
            acc_d[:, at] += _nn(dyx, hid)
            part = _nt(dg, wgu[0, :, at]) + _nt(du, wgu[1, :, at])
            db = part if db is None else db + part
        scatter.tile[...] = db.reshape(2, TB, DM)
        scatter.give(s)

        @pl.when((s == 13) | (s == 15))
        def _():
            n = jnp.clip(lax.div(s - 11, 2), 1, 2)
            rs[n - 1] = scatter.finish(n).astype(BF)
            home(n).start()

    lax.fori_loop(0, 16, step, None)
    scatter.settle(15)
    od_ref[...] = acc_d[...].T.astype(BF)
    rs[2] = scatter.finish(3).astype(BF)
    home(3).start()
    for k in FOUR:
        ogu_ref[k] = acc[:, pl.ds(pl.multiple_of(place(k) * ROWS, ROWS), ROWS), :].astype(BF)
    total = scatter.finish(0)
    for k in OTHERS:
        home(k).wait_recv()
        total += zr[k - 1].astype(F32)
    dh = own_dy_ref[...] + norm_back(h_ref[...], total.astype(BF).astype(F32)).astype(BF)
    dh_ref[...] = dh
    dhg[t] = dh
    spread = _Gather(d, t, dhg, *sems[4:])
    spread.start()
    for j in FOUR:
        if j:
            spread.relay(j)
        spread.arrived(j)
        chip = _chip(t, j)
        got = _nt(dhg[pl.ds(2 * chip, 2)].reshape(TILE, DM), wo[...]).astype(BF)
        for n in range(HEADS):
            out[j, n] = got[:, n * HEAD : (n + 1) * HEAD]
        pltpu.make_async_copy(out.at[j], do_ref.at[:, tokens(chip)], st.at[j]).start()
    whole = pltpu.make_async_copy(dhg, dhg_ref, st.at[4])
    whole.start()
    whole.wait()
    for j in FOUR:
        pltpu.make_async_copy(out.at[j], do_ref.at[:, tokens(_chip(t, j))], st.at[j]).wait()
    spread.close()
    scatter.close()
    for k in FOUR:
        gather(k).close()
        if k:
            along_z(k).wait_send()
            home(k).wait_send()


def mlp(b, h, wo, dy, dy_all, pieces, w_down):
    vmem = pl.BlockSpec(memory_space=VMEM)
    tile = lambda *lead: VMEM((*lead, TB, DM), BF)
    return pl.pallas_call(
        _mlp,
        in_specs=[HBM, vmem, HBM, vmem, *[HBM] * 6],
        out_specs=[vmem, HBM, HBM, vmem, vmem],
        out_shape=[jax.ShapeDtypeStruct((TB, DM), BF), jax.ShapeDtypeStruct((8, TB, DM), BF), jax.ShapeDtypeStruct((HEADS, SEQ, HEAD), BF),
                   jax.ShapeDtypeStruct((4, 2, ROWS, HU), BF), jax.ShapeDtypeStruct((HU, DM), BF)],
        scratch_shapes=[tile(4, 8), tile(8), VMEM((QC, DM), BF), VMEM((2, TILE, DM), BF), VMEM((2, DM, HU), BF), VMEM((HU, DM), BF),
                        VMEM((2, DM, HU), F32), VMEM((DM, HU), F32), tile(3), tile(3), VMEM((4, HEADS, TILE, HEAD), BF),
                        DMA((7,)), DMA((2,)), DMA((5,)), *[DMA((3,))] * 4, *_Gather.sems(4), *_Gather.sems(), *_Scatter.scratch(4)],
        compiler_params=_params(1),
        cost_estimate=pl.CostEstimate(flops=16 * TB * 4 * DM * HU * 16, transcendentals=0, bytes_accessed=32 * 2**20),
        name="mlp",
    )(b, h, wo, dy, dy_all, *pieces, w_down)


def shift(a, k):
    return lax.ppermute(a, "dp", [(n, (n + k) % 4) for n in FOUR])


def solution(mesh):
    def step(x, dy, wq, wk, wv, wo, w_gate, w_up, w_down):
        x, dy = x[0], dy[0]
        d = lax.axis_index("dp")
        gate_up = jnp.stack([w_gate, w_up])
        parts = [lax.dynamic_slice_in_dim(gate_up, lax.rem(d + n, 4) * HU, HU, 2) for n in FOUR]
        q, k, v, a, dy_all, weights, wo, cos, sin = into(normed(x), dy, wq, wk, wv, wo)
        q, parts = lax.optimization_barrier((q, parts))
        pieces = [parts[0]] + [shift(parts[4 - n], 4 - n) for n in OTHERS]
        o, lse = attend(q, k, v)
        h, b = between(o, wo, x)
        dh, dh_all, d_o, d_gate_up, d_down = mlp(b, h, wo, dy, dy_all.reshape(4, 4, TILE, DM), pieces, w_down)
        d_wo = jnp.einsum("htk,td->hkd", o, dh_all.reshape(SEQ, DM), preferred_element_type=F32).astype(BF).reshape(QC, DM)
        d_wo = lax.psum_scatter(d_wo, "dp", scatter_dimension=0, tiled=True)
        got = [d_gate_up[0]] + [shift(d_gate_up[n], n) for n in OTHERS]
        dq, dk, dv = attend_back(q, k, v, d_o, o, lse)
        dq, got, d_wo = lax.optimization_barrier((dq, got, d_wo))
        da, dw = outof(dq, dk, dv, a, weights, cos, sin)
        got = jnp.stack(got)
        d_gate, d_up = (jnp.concatenate([lax.dynamic_index_in_dim(got, lax.rem(d - j + 4, 4), 0, False)[n] for j in FOUR], 1) for n in (0, 1))
        dx = dh + norm_back(x, da.astype(BF).astype(F32)).astype(BF)
        return (dx[None], dw[0], dw[1], dw[2], d_wo, d_gate, d_up, d_down)

    states, by_columns, by_rows = P("dp", "tp", None), P("dp", "tp"), P(("tp", "dp"), None)
    weights = (by_columns, by_columns, by_columns, by_rows, by_columns, by_columns, by_rows)
    return jax.shard_map(step, mesh=mesh, in_specs=(states, states, *weights), out_specs=(states, *weights), check_vma=False)
```

```python
import functools

import jax
import jax.numpy as jnp
from jax import lax
from jax.experimental import pallas as pl
from jax.experimental.pallas import tpu as pltpu
from jax.sharding import PartitionSpec as P

NEG = -1e30
HIDDEN = 2 * NEG
LOG2E = 1.4426950408889634
HEAD = 128
THETA = 10000
MESH = pl.DeviceIdType.MESH
BF, F32 = jnp.bfloat16, jnp.float32
DMA, VMEM = pltpu.SemaphoreType.DMA, pltpu.VMEM
TB = 256
TILE = 2 * TB
SEQ = 2048
DM = 512
HEADS = 8
FEW = HEADS // 2
QC = HEADS * HEAD
HC = FEW * HEAD
HU = 1024
CH = 256
ROWS = 128
HBM = pl.BlockSpec(memory_space=pltpu.HBM)
LIMIT = 62 * 2**20
SOME = 24 * 2**20
SCALE = HEAD**-0.5
TOP = 3
FOUR = range(4)
OTHERS = (1, 2, 3)


def _nn(a, b):
    return lax.dot_general(a, b, (((1,), (0,)), ((), ())), preferred_element_type=F32)


def _nt(a, b):
    return lax.dot_general(a, b, (((1,), (1,)), ((), ())), preferred_element_type=F32)


def _inverse(wide):
    return lax.rsqrt(jnp.mean(wide**2, -1, keepdims=True) + 1e-6)


def normed(h):
    wide = h.astype(F32)
    return (wide * _inverse(wide)).astype(BF)


def norm_back(h, grad):
    wide = h.astype(F32)
    scale = _inverse(wide)
    unit = wide * scale
    return scale * (grad - unit * jnp.mean(grad * unit, -1, keepdims=True))


BLOCK = 512


def _seen(*shape):
    return lax.broadcasted_iota(jnp.int32, shape, 1) >= lax.broadcasted_iota(jnp.int32, shape, 0)


def _blocks(iq, block):
    lax.fori_loop(0, iq, lambda j, _: block(pl.multiple_of(j * BLOCK, BLOCK), BLOCK, 0, False), None)
    part = BLOCK // 2
    for at in (0, part):
        block(pl.multiple_of(iq * BLOCK + at, part), part, at, True)


def _forward(q_ref, k_ref, v_ref, o_ref, lse_ref, top_s, mix_s):
    heads = q_ref.shape[0]
    iq = pl.program_id(0)
    e = SCALE * LOG2E
    top_s[...] = jnp.full_like(top_s, NEG)
    mix_s[...] = jnp.zeros_like(mix_s)

    def block(start, keys, at, masked):
        here = pl.ds(start, keys)
        ones = jnp.ones((8, keys), BF)
        scores = [_nt(k_ref[i, here, :], q_ref[i, at:, :]) for i in range(heads)]
        ok = _seen(keys, BLOCK - at) if masked else None
        weights, keeps = [], []
        for i, s in enumerate(scores):
            if masked:
                s = jnp.where(ok, s, HIDDEN)
            old = top_s[i : i + 1, at:]
            top = jnp.maximum(old, s.max(axis=0, keepdims=True))
            top_s[i : i + 1, at:] = top
            weights.append(jnp.exp2((s - top) * e).astype(BF))
            keeps.append(jnp.exp2((old - top) * e))
        for i, (p, keep) in enumerate(zip(weights, keeps)):
            values = jnp.concatenate([v_ref[i, here, :].T, ones], axis=0)
            mix_s[i, :, at:] = mix_s[i, :, at:] * keep + _nn(values, p)

    _blocks(iq, block)
    for i in range(heads):
        total = mix_s[i, HEAD : HEAD + 1, :]
        o_ref[i] = (mix_s[i, :HEAD, :] * (1 / total)).T.astype(BF)
        lse_ref[i] = top_s[i : i + 1, :] * SCALE + jnp.log(total)


def attend(q, k, v):
    of_queries = pl.BlockSpec((HEADS, BLOCK, HEAD), lambda n: (0, n, 0))
    whole = pl.BlockSpec((HEADS, SEQ, HEAD), lambda n: (0, 0, 0))
    return pl.pallas_call(
        _forward,
        grid=(SEQ // BLOCK,),
        in_specs=[of_queries, whole, whole],
        out_specs=[of_queries, pl.BlockSpec((HEADS, 1, BLOCK), lambda n: (0, 0, n))],
        out_shape=[jax.ShapeDtypeStruct((HEADS, SEQ, HEAD), BF), jax.ShapeDtypeStruct((HEADS, 1, SEQ), F32)],
        scratch_shapes=[VMEM((HEADS, BLOCK), F32), VMEM((HEADS, HEAD + 8, BLOCK), F32)],
        compiler_params=pltpu.CompilerParams(dimension_semantics=("arbitrary",), vmem_limit_bytes=LIMIT),
        cost_estimate=pl.CostEstimate(flops=4 * HEADS * SEQ * SEQ * HEAD, transcendentals=HEADS * SEQ * SEQ, bytes_accessed=8 * HEADS * SEQ * HEAD),
        name="attend",
    )(q, k, v)


def _backward(q_ref, k_ref, v_ref, do_ref, o_ref, lse_ref, dq_ref, dk_ref, dv_ref, dq_s, dk_s, dv_s):
    heads = q_ref.shape[0]
    iq = pl.program_id(0)
    e = SCALE * LOG2E

    @pl.when(iq == 0)
    def _():
        dk_s[...] = jnp.zeros_like(dk_s)
        dv_s[...] = jnp.zeros_like(dv_s)

    dq_s[...] = jnp.zeros_like(dq_s)
    lses = [lse_ref[i] * LOG2E for i in range(heads)]
    deltas = [(do_ref[i].astype(F32) * o_ref[i].astype(F32)).T.sum(0, keepdims=True) for i in range(heads)]

    def block(start, keys, at, masked):
        here = pl.ds(start, keys)
        scores = [_nt(k_ref[i, here, :], q_ref[i, at:, :]) for i in range(heads)]
        dps = [_nt(v_ref[i, here, :], do_ref[i, at:, :]) for i in range(heads)]
        ok = _seen(keys, BLOCK - at) if masked else None
        for i in range(heads):
            p = jnp.exp2(scores[i] * e - lses[i][:, at:])
            if masked:
                p = jnp.where(ok, p, 0.0)
            ds = (p * (dps[i] - deltas[i][:, at:])).astype(BF)
            dv_s[i, here, :] += _nn(p.astype(BF), do_ref[i, at:, :])
            dk_s[i, here, :] += _nn(ds, q_ref[i, at:, :])
            dq_s[i, :, at:] += _nn(k_ref[i, here, :].T, ds)

    _blocks(iq, block)
    for i in range(heads):
        dq_ref[i] = (dq_s[i] * SCALE).T.astype(BF)

    @pl.when(iq == pl.num_programs(0) - 1)
    def _():
        dk_ref[...] = (dk_s[...] * SCALE).astype(BF)
        dv_ref[...] = dv_s[...].astype(BF)


def attend_back(q, k, v, d_out, out, lse, part):
    of_queries = lambda part: pl.BlockSpec((FEW, BLOCK, HEAD), lambda n: (part, n, 0))
    whole = lambda part: pl.BlockSpec((FEW, SEQ, HEAD), lambda n: (part, 0, 0))
    return pl.pallas_call(
        _backward,
        grid=(SEQ // BLOCK,),
        in_specs=[of_queries(part), whole(part), whole(part), of_queries(part), of_queries(part), pl.BlockSpec((FEW, 1, BLOCK), lambda n: (part, 0, n))],
        out_specs=[of_queries(0), whole(0), whole(0)],
        out_shape=[jax.ShapeDtypeStruct((FEW, SEQ, HEAD), BF)] * 3,
        scratch_shapes=[VMEM((FEW, HEAD, BLOCK), F32), VMEM((FEW, SEQ, HEAD), F32), VMEM((FEW, SEQ, HEAD), F32)],
        compiler_params=pltpu.CompilerParams(dimension_semantics=("arbitrary",), vmem_limit_bytes=LIMIT),
        cost_estimate=pl.CostEstimate(flops=10 * FEW * SEQ * SEQ * HEAD, transcendentals=FEW * SEQ * SEQ, bytes_accessed=18 * FEW * SEQ * HEAD),
        name="attend_back",
    )(q, k, v, d_out, out, lse)


def _flip(a, by):
    return a + by - 2 * a * by


def _chip(t, j):
    x, y = lax.div(t, 4), lax.rem(lax.div(t, 2), 2)
    return 2 * _flip(x, lax.div(j, 2)) + _flip(y, lax.rem(j, 2))


def _send(src, dst, s, r, to):
    return pltpu.make_async_remote_copy(src_ref=src, dst_ref=dst, send_sem=s, recv_sem=r, device_id=to, device_id_type=MESH)


def _meet(d, t):
    core = lax.rem(t, 2)
    barrier = pltpu.get_barrier_semaphore()
    for k in range(1, 4):
        pl.semaphore_signal(barrier, inc=1, device_id=(lax.rem(d + k, 4), t), device_id_type=MESH)
        pl.semaphore_signal(barrier, inc=1, device_id=(d, 2 * _chip(t, k) + core), device_id_type=MESH)
    pl.semaphore_signal(barrier, inc=1, device_id=(d, t + 1 - 2 * core), device_id_type=MESH)
    pl.semaphore_wait(barrier, 7)


def _params(number):
    return pltpu.CompilerParams(collective_id=number, has_side_effects=True, vmem_limit_bytes=LIMIT)


class _Gather:
    @staticmethod
    def sems(*lead):
        return [DMA((*lead, n)) for n in (3, 3, 4, 4)]

    def __init__(self, d, t, slots, xs, xr, cs, cr):
        core = lax.rem(t, 2)
        peer = lambda j: 2 * _chip(t, j) + core
        self.across = lambda j: _send(slots.at[t], slots.at[t], xs.at[j - 1], xr.at[j - 1], (d, peer(j)))
        self.to_mate = lambda j: _send(slots.at[peer(j)], slots.at[peer(j)], cs.at[j], cr.at[j], (d, t + 1 - 2 * core))

    def start(self):
        for j in OTHERS[::-1]:
            self.across(j).start()
        self.to_mate(0).start()

    def relay(self, j):
        self.across(j).wait_recv()
        self.to_mate(j).start()

    def arrived(self, j):
        self.to_mate(j).wait_recv()

    def close(self):
        for j in FOUR:
            self.to_mate(j).wait_send()
            if j:
                self.across(j).wait_send()


class _Scatter:
    @staticmethod
    def scratch(n):
        tile = lambda *lead: VMEM((*lead, TB, DM), BF)
        return [VMEM((2, TB, DM), F32), VMEM((TB, DM), F32), VMEM((n, TB, DM), F32), tile(4 * n), tile(4 * n), tile(n, 3), tile(n, 3),
                DMA((4 * n,)), DMA((4 * n,)), DMA((n, 3)), DMA((n, 3))]

    def __init__(self, d, t, n, tile, mine, keep, ps, cr, qs, xr, p_s, p_r, q_s, q_r):
        self.core = core = lax.rem(t, 2)
        self.n, self.tile, self.mine, self.keep, self.ps, self.cr, self.qs, self.xr = n, tile, mine, keep, ps, cr, qs, xr
        self.half = lambda s: _send(ps.at[s], cr.at[s], p_s.at[s], p_r.at[s], (d, t + 1 - 2 * core))
        self.quarter = lambda k, j: _send(qs.at[k, j - 1], xr.at[k, j - 1], q_s.at[k, j - 1], q_r.at[k, j - 1], (d, 2 * _chip(t, j) + core))

    def give(self, s, first=0):
        @pl.when(s > first)
        def _():
            self.settle(jnp.maximum(s - 1, first))

        self.ps[s] = self.tile[1 - self.core].astype(BF)
        self.half(s).start()
        self.mine[...] = self.tile[self.core]

    def settle(self, s):
        k, j = lax.div(s, 4), TOP - lax.rem(s, 4)
        self.half(s).wait_recv()
        total = self.mine[...] + self.cr[s].astype(F32)

        @pl.when(j > 0)
        def _():
            self.qs[k, jnp.maximum(j - 1, 0)] = total.astype(BF)
            self.quarter(k, jnp.maximum(j, 1)).start()

        @pl.when(j == 0)
        def _():
            self.keep[k] = total

    def finish(self, k):
        total = self.keep[k]
        for j in OTHERS:
            self.quarter(k, j).wait_recv()
            total += self.xr[k, j - 1].astype(F32)
        return total

    def close(self):
        for k in range(self.n):
            for j in OTHERS:
                self.quarter(k, j).wait_send()
            for i in FOUR:
                self.half(4 * k + i).wait_send()


def _spun(t, cos, sin):
    return t * cos + pltpu.roll(t, HEAD // 2, 1) * sin


def _into(a_ref, dy_ref, wq_ref, wk_ref, wv_ref, wo_ref, freq_ref, q_ref, k_ref, v_ref, ag_ref, dg_ref, wf_ref, of_ref, cos_ref, sin_ref,
          ag, dg, wf, of, cos, sin, out, ld, st, os, up_s, up_r, dn_s, dn_r, *sems):
    d, t = lax.axis_index("dp"), lax.axis_index("tp")
    of_a, of_dy = sems[:4], sems[4:]
    gather = _Gather(d, t, ag, *of_a)
    spread = lambda o: _Gather(d, t, dg.at[o], *(x.at[o] for x in of_dy))

    def block(m, o):
        if m == 0:
            return dg.at[o, t]
        step = TB if m == 4 else ROWS
        rows = pl.ds(pl.multiple_of(o * step, step), step)
        return of.at[rows] if m == 4 else wf.at[m - 1, rows]

    parts = range(5)
    loads = [pltpu.make_async_copy(source, block(m, d), ld.at[m]) for m, source in enumerate((dy_ref, wq_ref, wk_ref, wv_ref, wo_ref))]
    loads += [pltpu.make_async_copy(a_ref, ag.at[t], ld.at[5])]
    for copy in loads:
        copy.start()
    up = lambda m, o: _send(block(m, o), block(m, o), up_s.at[m, o], up_r.at[m, o], (jnp.minimum(d + 1, TOP), t))
    down = lambda m, o: _send(block(m, o), block(m, o), dn_s.at[m, o], dn_r.at[m, o], (jnp.maximum(d - 1, 0), t))
    _meet(d, t)
    for m in parts:
        loads[m].wait()

        @pl.when(d < TOP)
        def _():
            up(m, d).start()

        @pl.when(d > 0)
        def _():
            down(m, d).start()

    loads[5].wait()
    gather.start()
    spread(d).start()
    angle = lax.broadcasted_iota(jnp.int32, (SEQ, HEAD), 0).astype(F32) * freq_ref[...]
    cos[...] = jnp.cos(angle)
    sin[...] = jnp.where(lax.broadcasted_iota(jnp.int32, (SEQ, HEAD), 1) < HEAD // 2, -1.0, 1.0) * jnp.sin(angle)
    leaving = [pltpu.make_async_copy(cos, cos_ref, st.at[0]), pltpu.make_async_copy(sin, sin_ref, st.at[1])]
    for copy in leaving:
        copy.start()

    def whole(source, target, n):
        leaving.append(pltpu.make_async_copy(source, target, st.at[n]))
        leaving[-1].start()

    tokens = lambda n: pl.ds(pl.multiple_of(n * TILE, TILE), TILE)
    targets = (None, q_ref, k_ref, v_ref)
    leave = lambda m, n: pltpu.make_async_copy(out.at[m - 1, :, tokens(n)], targets[m].at[:, tokens(n)], os.at[m - 1, n])

    def multiply(m):
        def tile(n, _):
            got = _nn(ag[pl.ds(2 * n, 2)].reshape(TILE, DM), wf[m - 1]).astype(BF)
            for h in range(HEADS):
                piece = got[:, h * HEAD : (h + 1) * HEAD]
                if m < 3:
                    piece = _spun(piece.astype(F32), cos[tokens(n), :], sin[tokens(n), :]).astype(BF)
                out[m - 1, h, tokens(n), :] = piece
            leave(m, n).start()

        lax.fori_loop(0, 4, tile, None)

    for j in OTHERS:
        gather.relay(j)
    for j in FOUR:
        gather.arrived(j)
    whole(ag, ag_ref, 2)
    def share():
        for j in OTHERS:
            spread(d).relay(j)
        for far in OTHERS:
            for on, o in ((d >= far, jnp.maximum(d - far, 0)), (d + far <= TOP, jnp.minimum(d + far, TOP))):

                @pl.when(on)
                def _():
                    for j in OTHERS:
                        spread(o).relay(j)

        for o in FOUR:
            for j in FOUR:
                spread(o).arrived(j)
        whole(dg, dg_ref, 5)

    for far in OTHERS:
        below, above = jnp.maximum(d - far, 0), jnp.minimum(d + far, TOP)
        for m in parts:
            if far == TOP and m == 4:
                share()

            @pl.when(d >= far)
            def _():
                up(m, below).wait_recv()

                @pl.when(d < TOP)
                def _():
                    up(m, below).start()

                if m == 0:
                    spread(below).start()

            @pl.when(d + far <= TOP)
            def _():
                down(m, above).wait_recv()

                @pl.when(d > 0)
                def _():
                    down(m, above).start()

                if m == 0:
                    spread(above).start()

            if far == 3 and 0 < m < 4:
                multiply(m)
    whole(wf, wf_ref, 3)
    whole(of, of_ref, 4)
    for m in parts:
        if 0 < m < 4:
            for n in FOUR:
                leave(m, n).wait()
        for o in FOUR:

            @pl.when((o <= d) & (d < TOP))
            def _():
                up(m, o).wait_send()

            @pl.when((o >= d) & (d > 0))
            def _():
                down(m, o).wait_send()

    for copy in leaving:
        copy.wait()
    gather.close()
    for o in FOUR:
        spread(o).close()


def into(a, dy, wq, wk, wv, wo):
    freq = (THETA ** (-(jnp.arange(HEAD, dtype=F32) % (HEAD // 2)) / (HEAD // 2)))[None]
    heads = jax.ShapeDtypeStruct((HEADS, SEQ, HEAD), BF)
    table = jax.ShapeDtypeStruct((SEQ, HEAD), F32)
    shapes = (8, TB, DM), (4, 8, TB, DM), (3, DM, QC), (QC, DM)
    return pl.pallas_call(
        _into,
        in_specs=[HBM] * 6 + [pl.BlockSpec(memory_space=VMEM)],
        out_specs=[HBM] * 9,
        out_shape=[heads, heads, heads, *[jax.ShapeDtypeStruct(shape, BF) for shape in shapes], table, table],
        scratch_shapes=[*[VMEM(shape, BF) for shape in shapes], VMEM((SEQ, HEAD), F32), VMEM((SEQ, HEAD), F32), VMEM((3, HEADS, SEQ, HEAD), BF),
                        DMA((6,)), DMA((6,)), DMA((3, 4)), *[DMA((5, 4))] * 4, *_Gather.sems(), *_Gather.sems(4)],
        compiler_params=_params(0),
        cost_estimate=pl.CostEstimate(flops=6 * SEQ * DM * QC, transcendentals=0, bytes_accessed=SOME),
        name="into",
    )(a, dy, wq, wk, wv, wo, freq)


def _weigh(m, grads, at, ag, cos, sin, acc):
    acc[m] = jnp.zeros_like(acc[m])

    def tile(n, _):
        place = pl.ds(pl.multiple_of(n * TILE, TILE), TILE)
        pieces = []
        for h in range(FEW):
            piece = grads[m, at + h, place, :]
            if m < 2:
                piece = _spun(piece.astype(F32), cos[place, :], -sin[place, :]).astype(BF)
                grads[m, at + h, place, :] = piece
            pieces.append(piece)
        acc[m] += _nn(ag[pl.ds(2 * n, 2)].reshape(TILE, DM).T, jnp.concatenate(pieces, 1))

    lax.fori_loop(0, 4, tile, None)


def _first(dq_ref, dk_ref, dv_ref, ag_ref, cos_ref, sin_ref, turned_ref, dw_ref, grads, ag, cos, sin, acc, ld, st):
    loads = [pltpu.make_async_copy(s, to, ld.at[n]) for n, (s, to) in enumerate(
        [(dq_ref, grads.at[0]), (ag_ref, ag), (cos_ref, cos), (sin_ref, sin), (dk_ref, grads.at[1]), (dv_ref, grads.at[2])])]
    leave = lambda m: pltpu.make_async_copy(grads.at[m], turned_ref.at[m], st.at[m])
    for copy in loads:
        copy.start()
    for copy in loads[:4]:
        copy.wait()
    for m in range(3):
        if m:
            loads[3 + m].wait()
        _weigh(m, grads, 0, ag, cos, sin, acc)
        leave(m).start()
        dw_ref[:, m * HC : (m + 1) * HC] = acc[m].astype(BF)
    for m in range(3):
        leave(m).wait()


def first(dq, dk, dv, a, cos, sin):
    return pl.pallas_call(
        _first,
        in_specs=[HBM] * 6,
        out_specs=[HBM, pl.BlockSpec(memory_space=VMEM)],
        out_shape=[jax.ShapeDtypeStruct((3, FEW, SEQ, HEAD), BF), jax.ShapeDtypeStruct((DM, 3 * HC), BF)],
        scratch_shapes=[VMEM((3, FEW, SEQ, HEAD), BF), VMEM((8, TB, DM), BF), VMEM((SEQ, HEAD), F32), VMEM((SEQ, HEAD), F32), VMEM((3, DM, HC), F32),
                        DMA((6,)), DMA((3,))],
        compiler_params=pltpu.CompilerParams(vmem_limit_bytes=LIMIT),
        cost_estimate=pl.CostEstimate(flops=6 * SEQ * DM * HC, transcendentals=0, bytes_accessed=SOME),
        name="first",
    )(dq, dk, dv, a, cos, sin)


def _outof(done_ref, dq_ref, dk_ref, dv_ref, ag_ref, wf_ref, cos_ref, sin_ref, x_ref, dh_ref, dx_ref, *rest):
    dw_refs = rest[:3]
    (grads, ag, wf, cos, sin, acc, us, ds, ur, dr, ld, up_s, up_r, dn_s, dn_r, *sums) = rest[3:]
    d, t = lax.axis_index("dp"), lax.axis_index("tp")
    scatter = _Scatter(d, t, 1, *sums)
    late = lambda m: grads.at[m, pl.ds(FEW, FEW)]
    loads = [pltpu.make_async_copy(s, to, ld.at[n]) for n, (s, to) in enumerate(
        [(dq_ref, late(0)), (ag_ref, ag), (cos_ref, cos), (sin_ref, sin), (dk_ref, late(1)), (dv_ref, late(2)), (wf_ref, wf),
         *[(done_ref.at[m], grads.at[m, pl.ds(0, FEW)]) for m in range(3)]])]
    for copy in loads:
        copy.start()
    up = lambda m, p: _send(us.at[m, p], ur.at[m, p], up_s.at[m, p], up_r.at[m, p], (jnp.minimum(d + 1, TOP), t))
    down = lambda m, p: _send(ds.at[m, p], dr.at[m, p], dn_s.at[m, p], dn_r.at[m, p], (jnp.maximum(d - 1, 0), t))
    rows = lambda p: slice(p * ROWS, (p + 1) * ROWS)

    def begin(m, n):
        @pl.when(d == 0)
        def _():
            us[m, TOP - n] = acc[m, rows(TOP - n), :].astype(BF)
            up(m, TOP - n).start()

        @pl.when(d == TOP)
        def _():
            ds[m, n] = acc[m, rows(n), :].astype(BF)
            down(m, n).start()

    _meet(d, t)
    for copy in loads[:4]:
        copy.wait()
    for m in range(3):
        if m:
            loads[3 + m].wait()
        _weigh(m, grads, FEW, ag, cos, sin, acc)

        begin(m, 0)
    for n in (1, 2):
        for m in range(3):
            begin(m, n)

    def pass_on(n):
        p, o = TOP - n, n
        for m in range(3):

            @pl.when((d > 0) & (d < p))
            def _():
                up(m, p).wait_recv()
                us[m, p] = (acc[m, rows(p), :] + ur[m, p].astype(F32)).astype(BF)
                up(m, p).start()

            @pl.when((d < TOP) & (d > o))
            def _():
                down(m, o).wait_recv()
                ds[m, o] = (acc[m, rows(o), :] + dr[m, o].astype(F32)).astype(BF)
                down(m, o).start()

    for copy in loads[6:]:
        copy.wait()
    pass_on(0)

    def for_a(s, _):
        place = pl.ds(pl.multiple_of(_chip(t, TOP - s) * TILE, TILE), TILE)
        total = sum(_nt(jnp.concatenate([grads[m, h, place, :] for h in range(HEADS)], 1), wf[m]) for m in range(3))
        scatter.tile[...] = total.reshape(2, TB, DM)
        scatter.give(s)

    lax.fori_loop(0, 4, for_a, None)
    scatter.settle(3)
    pass_on(1)
    da = scatter.finish(0).astype(BF).astype(F32)
    dx_ref[...] = dh_ref[...] + norm_back(x_ref[...], da).astype(BF)
    own = pl.ds(pl.multiple_of(d * ROWS, ROWS), ROWS)
    for m in range(3):

        @pl.when(d > 0)
        def _():
            up(m, d).wait_recv()
            acc[m, own, :] += ur[m, d].astype(F32)

        @pl.when(d < TOP)
        def _():
            down(m, d).wait_recv()
            acc[m, own, :] += dr[m, d].astype(F32)

        dw_refs[m][...] = acc[m, own, :].astype(BF)
        for p in FOUR:

            @pl.when(d < p)
            def _():
                up(m, p).wait_send()

            @pl.when(d > p)
            def _():
                down(m, p).wait_send()

    scatter.close()


def outof(done, dq, dk, dv, a, weights, cos, sin, x, dh):
    vmem = pl.BlockSpec(memory_space=VMEM)
    return pl.pallas_call(
        _outof,
        in_specs=[*[HBM] * 8, vmem, vmem],
        out_specs=[vmem] * 4,
        out_shape=[jax.ShapeDtypeStruct((TB, DM), BF), *[jax.ShapeDtypeStruct((ROWS, HC), BF)] * 3],
        scratch_shapes=[VMEM((3, HEADS, SEQ, HEAD), BF), VMEM((8, TB, DM), BF), VMEM((3, DM, QC), BF), VMEM((SEQ, HEAD), F32), VMEM((SEQ, HEAD), F32),
                        VMEM((3, DM, HC), F32), *[VMEM((3, 4, ROWS, HC), BF)] * 4, DMA((10,)), *[DMA((3, 4))] * 4, *_Scatter.scratch(1)],
        compiler_params=_params(2),
        cost_estimate=pl.CostEstimate(flops=9 * SEQ * DM * QC, transcendentals=0, bytes_accessed=SOME),
        name="outof",
    )(done, dq, dk, dv, a, weights, cos, sin, x, dh)


def _between(o_ref, wo_ref, x_ref, h_ref, b_ref, wo, ob, ld, o_m, *sums):
    d, t = lax.axis_index("dp"), lax.axis_index("tp")
    scatter = _Scatter(d, t, 1, *sums)
    load = pltpu.make_async_copy(wo_ref, wo, ld.at[0])

    def fetch(i):
        tokens = pl.ds(pl.multiple_of(_chip(t, 3 - i) * TILE, TILE), TILE)
        return pltpu.make_async_copy(o_ref.at[:, tokens], ob.at[i], o_m.at[i])

    load.start()
    for i in FOUR:
        fetch(i).start()
    _meet(d, t)
    load.wait()

    def tile(i, _):
        fetch(i).wait()
        heads = jnp.concatenate([ob[i, h] for h in range(HEADS)], 1)
        scatter.tile[...] = _nn(heads, wo[...]).reshape(2, TB, DM)
        scatter.give(i)

    lax.fori_loop(0, 4, tile, None)
    scatter.settle(3)
    h = x_ref[...] + scatter.finish(0).astype(BF)
    h_ref[...] = h
    b_ref[...] = normed(h)
    scatter.close()


def between(o, wo, x):
    vmem = pl.BlockSpec(memory_space=VMEM)
    return pl.pallas_call(
        _between,
        in_specs=[HBM, HBM, vmem],
        out_specs=[vmem, vmem],
        out_shape=[jax.ShapeDtypeStruct((TB, DM), BF)] * 2,
        scratch_shapes=[VMEM((QC, DM), BF), VMEM((4, HEADS, TILE, HEAD), BF), DMA((1,)), DMA((4,)), *_Scatter.scratch(1)],
        compiler_params=_params(3),
        cost_estimate=pl.CostEstimate(flops=2 * SEQ * DM * QC, transcendentals=0, bytes_accessed=SOME),
        name="between",
    )(o, wo, x)


def _mlp(b_ref, h_ref, wo_ref, own_dy_ref, dy_ref, *rest):
    pieces, wd_ref = rest[:4], rest[4]
    dh_ref, dhg_ref, do_ref, od_ref, *grads = rest[5:13]
    (g, dhg, wo, dyb, wgu, wd, acc, acc_d, rs, zr, out, ld, dy_m, st, zs_s, zs_r, r_s, r_r) = rest[13:31]
    sems, sums = rest[31:39], rest[39:]
    d, t = lax.axis_index("dp"), lax.axis_index("tp")
    place = lambda k: lax.rem(d + k, 4)
    scatter = _Scatter(d, t, 4, *sums)
    along_z = lambda k: _send(g.at[0, t], g.at[k, t], zs_s.at[k - 1], zs_r.at[k - 1], (lax.rem(d - k + 4, 4), t))
    gather = lambda k: _Gather(d, t, g.at[k], *(x.at[k] for x in sems[:4]))
    home = lambda k: _send(rs.at[k - 1], zr.at[k - 1], r_s.at[k - 1], r_r.at[k - 1], (place(k), t))
    tokens = lambda chip: pl.ds(pl.multiple_of(chip * TILE, TILE), TILE)

    def fetch(s):
        k, j = lax.div(s, 4), TOP - lax.rem(s, 4)
        return pltpu.make_async_copy(dy_ref.at[place(k), _chip(t, j)], dyb.at[lax.rem(s, 2)], dy_m.at[lax.rem(s, 2)])

    loads = [pltpu.make_async_copy(b_ref, g.at[0, t], ld.at[0]), pltpu.make_async_copy(wd_ref, wd, ld.at[1])]
    for k in FOUR:
        rows = pl.ds(pl.multiple_of(place(k) * ROWS, ROWS), ROWS)
        loads += [pltpu.make_async_copy(pieces[k], wgu.at[:, rows], ld.at[2 + k])]
    loads += [pltpu.make_async_copy(wo_ref, wo, ld.at[6])]
    for copy in loads:
        copy.start()
    fetch(0).start()
    _meet(d, t)
    loads[0].wait()
    gather(0).start()
    for k in OTHERS:
        along_z(k).start()
    acc[...] = jnp.zeros_like(acc)
    acc_d[...] = jnp.zeros_like(acc_d)
    along_z(1).wait_recv()
    gather(1).start()
    for copy in loads[1:]:
        copy.wait()
    for j in OTHERS:
        gather(0).relay(j)

    def step(s, _):
        k, i = lax.div(s, 4), lax.rem(s, 4)
        chip = _chip(t, 3 - i)
        after = jnp.minimum(k + 1, 3)

        @pl.when(i == 0)
        def _():
            for n in FOUR:
                gather(k).arrived(n)

        @pl.when((s == 1) | (s == 2))
        def _():
            n = jnp.clip(s + 1, 2, 3)
            along_z(n).wait_recv()
            gather(n).start()

        @pl.when((i == 3) & (k < TOP))
        def _():
            for n in OTHERS:
                gather(after).relay(n)

        @pl.when(s < 15)
        def _():
            fetch(s + 1).start()

        fetch(s).wait()
        bt = g[k, pl.ds(2 * chip, 2)].reshape(TILE, DM)
        dyt = dyb[lax.rem(s, 2)]
        bx, dyx = bt.T, dyt.T
        db = None
        for n in range(HU // CH):
            at = slice(n * CH, (n + 1) * CH)
            gate, up = _nn(bt, wgu[0, :, at]), _nn(bt, wgu[1, :, at])
            dh = _nt(dyt, wd[at, :]).astype(BF).astype(F32)
            sig = 1 / (1 + jnp.exp(-gate))
            act = gate * sig
            hid = (act * up).astype(BF)
            du = (dh * act).astype(BF)
            dg = (dh * up * (sig * (1 + gate * (1 - sig)))).astype(BF)
            acc[0, :, at] += _nn(bx, dg)
            acc[1, :, at] += _nn(bx, du)
            acc_d[:, at] += _nn(dyx, hid)
            part = _nt(dg, wgu[0, :, at]) + _nt(du, wgu[1, :, at])
            db = part if db is None else db + part
        scatter.tile[...] = db.reshape(2, TB, DM)
        scatter.give(s)

        @pl.when((s == 13) | (s == 15))
        def _():
            n = jnp.clip(lax.div(s - 11, 2), 1, 2)
            rs[n - 1] = scatter.finish(n).astype(BF)
            home(n).start()

    lax.fori_loop(0, 16, step, None)
    scatter.settle(15)
    od_ref[...] = acc_d[...].T.astype(BF)
    rs[2] = scatter.finish(3).astype(BF)
    home(3).start()
    for k in FOUR:
        grads[k][...] = acc[:, pl.ds(pl.multiple_of(place(k) * ROWS, ROWS), ROWS), :].astype(BF)
    total = scatter.finish(0)
    for k in OTHERS:
        home(k).wait_recv()
        total += zr[k - 1].astype(F32)
    dh = own_dy_ref[...] + norm_back(h_ref[...], total.astype(BF).astype(F32)).astype(BF)
    dh_ref[...] = dh
    dhg[t] = dh
    spread = _Gather(d, t, dhg, *sems[4:])
    spread.start()
    for j in FOUR:
        if j:
            spread.relay(j)
        spread.arrived(j)
        chip = _chip(t, j)
        got = _nt(dhg[pl.ds(2 * chip, 2)].reshape(TILE, DM), wo[...]).astype(BF)
        for n in range(HEADS):
            out[j, n] = got[:, n * HEAD : (n + 1) * HEAD]
        pltpu.make_async_copy(out.at[j], do_ref.at[:, tokens(chip)], st.at[j]).start()
    whole = pltpu.make_async_copy(dhg, dhg_ref, st.at[4])
    whole.start()
    whole.wait()
    for j in FOUR:
        pltpu.make_async_copy(out.at[j], do_ref.at[:, tokens(_chip(t, j))], st.at[j]).wait()
    spread.close()
    scatter.close()
    for k in FOUR:
        gather(k).close()
        if k:
            along_z(k).wait_send()
            home(k).wait_send()


def mlp(b, h, wo, dy, dy_all, pieces, w_down):
    vmem = pl.BlockSpec(memory_space=VMEM)
    tile = lambda *lead: VMEM((*lead, TB, DM), BF)
    return pl.pallas_call(
        _mlp,
        in_specs=[HBM, vmem, HBM, vmem, *[HBM] * 6],
        out_specs=[vmem, HBM, HBM, *[vmem] * 5],
        out_shape=[jax.ShapeDtypeStruct((TB, DM), BF), jax.ShapeDtypeStruct((8, TB, DM), BF), jax.ShapeDtypeStruct((HEADS, SEQ, HEAD), BF),
                   jax.ShapeDtypeStruct((HU, DM), BF), *[jax.ShapeDtypeStruct((2, ROWS, HU), BF)] * 4],
        scratch_shapes=[tile(4, 8), tile(8), VMEM((QC, DM), BF), VMEM((2, TILE, DM), BF), VMEM((2, DM, HU), BF), VMEM((HU, DM), BF),
                        VMEM((2, DM, HU), F32), VMEM((DM, HU), F32), tile(3), tile(3), VMEM((4, HEADS, TILE, HEAD), BF),
                        DMA((7,)), DMA((2,)), DMA((5,)), *[DMA((3,))] * 4, *_Gather.sems(4), *_Gather.sems(), *_Scatter.scratch(4)],
        compiler_params=_params(1),
        cost_estimate=pl.CostEstimate(flops=16 * TB * 4 * DM * HU * 16, transcendentals=0, bytes_accessed=SOME),
        name="mlp",
    )(b, h, wo, dy, dy_all, *pieces, w_down)


def shift(a, k):
    return lax.ppermute(a, "dp", [(n, (n + k) % 4) for n in FOUR])


def solution(mesh):
    def step(x, dy, wq, wk, wv, wo, w_gate, w_up, w_down):
        x, dy = x[0], dy[0]
        d = lax.axis_index("dp")
        gate_up = jnp.stack([w_gate, w_up])
        parts = [lax.dynamic_slice_in_dim(gate_up, lax.rem(d + n, 4) * HU, HU, 2) for n in FOUR]
        q, k, v, a, dy_all, weights, wo, cos, sin = into(normed(x), dy, wq, wk, wv, wo)
        q, parts = lax.optimization_barrier((q, parts))
        pieces = [parts[0]] + [shift(parts[4 - n], 4 - n) for n in OTHERS]
        o, lse = attend(q, k, v)
        h, b = between(o, wo, x)
        dh, dh_all, d_o, d_down, *d_gate_up = mlp(b, h, wo, dy, dy_all.reshape(4, 4, TILE, DM), pieces, w_down)
        d_wo = jnp.einsum("htk,td->hkd", o, dh_all.reshape(SEQ, DM), preferred_element_type=F32).astype(BF).reshape(QC, DM)
        d_wo = lax.psum_scatter(d_wo, "dp", scatter_dimension=0, tiled=True)
        got = [d_gate_up[0]] + [shift(d_gate_up[n], n) for n in OTHERS]
        early = attend_back(q, k, v, d_o, o, lse, 0)
        early, got[1], got[3] = lax.optimization_barrier((early, got[1], got[3]))
        done, dw_first = first(*early, a, cos, sin)
        d_o, dw_first = lax.optimization_barrier((d_o, dw_first))
        dw_first = lax.psum_scatter(dw_first, "dp", scatter_dimension=0, tiled=True)
        dq, dk, dv = attend_back(q, k, v, d_o, o, lse, 1)
        dq, got, d_wo = lax.optimization_barrier((dq, got, d_wo))
        dx, *dw = outof(done, dq, dk, dv, a, weights, cos, sin, x, dh)
        dw = [jnp.concatenate([dw_first[:, n * HC : (n + 1) * HC], late], 1) for n, late in enumerate(dw)]
        got = jnp.stack(got)
        d_gate, d_up = (jnp.concatenate([lax.dynamic_index_in_dim(got, lax.rem(d - j + 4, 4), 0, False)[n] for j in FOUR], 1) for n in (0, 1))
        return (dx[None], *dw, d_wo, d_gate, d_up, d_down)

    states, by_columns, by_rows = P("dp", "tp", None), P("dp", "tp"), P(("tp", "dp"), None)
    weights = (by_columns, by_columns, by_columns, by_rows, by_columns, by_columns, by_rows)
    return jax.shard_map(step, mesh=mesh, in_specs=(states, states, *weights), out_specs=(states, *weights), check_vma=False)
```
